32 devices in a mesh: section: 4 (over z), mp: 4 (over y, core), dp: 2 (over x).
Axes of the slice: x: 2, y: 2, z: 4, core: 2. Of those that a mesh axis runs over, the one named last changes fastest.
Arguments:
- context: bfloat16 [4, 1024, 6144], P('section', None, 'mp'), may hold values from -6 to 6
- out_weight: bfloat16 [4, 6144, 4, 2, 1536], P('section', 'mp', None, 'dp'), may hold values from -0.078125 to 0.078125
- residual: bfloat16 [4, 1024, 12288], P('section', None, ('mp', 'dp')), may hold values from -6 to 6
- layer_norm_gain: float32 [4, 12288], P('section', 'mp'), may hold values from 0.25 to 1.75
- layer_norm_bias: float32 [4, 12288], P('section', 'mp'), may hold values from -3 to 3
- ln_cotangent: bfloat16 [4, 1024, 12288], P('section', 'dp', 'mp'), may hold values from -6 to 6
Outputs:
- layer_norm_output: bfloat16 [4, 1024, 12288], P('section', 'dp', 'mp')
- resid_grad: bfloat16 [4, 1024, 12288], P('section', 'dp', 'mp')
The draws below stay inside these ranges and needn't reach their ends.
All inputs are finite; a program needn't handle non-finite values.
Results may differ from the reference program's by a relative error of at most 0.0047.
Values may be sent and summed in bfloat16 or wider, within the bound.
A program may use at most 128 MiB of HBM per device.

```python
import jax
import jax.numpy as jnp
from jax import lax

D = 12288
TOK = 1024
HD = 6144
DB = 1536
SECTIONS = 4
N_MP = 4
N_DP = 2


def block_scale(stream_key, dims, split, least, top_value):
    def one(axis_at, shards_of):
        heights = jax.random.uniform(jax.random.fold_in(jax.random.fold_in(stream_key, 6), axis_at), (shards_of,), jnp.float32, least / len(split), top_value / len(split))
        return jnp.repeat(jnp.exp(heights), dims[axis_at] // shards_of).reshape((-1,) + (1,) * (len(dims) - axis_at - 1))

    gain = one(*split[0])
    for cut in split[1:]:
        gain = gain * one(*cut)
    return gain


def normal_values(rng, dims, spread, most, split=(), held_as=jnp.bfloat16):
    gain = block_scale(rng, dims, split, -0.22, 0.18) if split else 1.0
    entries = jax.random.normal(rng, dims, jnp.float32) * spread * gain
    return jnp.minimum(jnp.maximum(entries, -most), most).astype(held_as)


def setup_inputs(seed: int = 0) -> dict:
    key_of = jax.random.split(jax.random.key(seed), 7)
    context = normal_values(key_of[0], (SECTIONS, TOK, HD), 1.0, 6.0, ((0, 4), (2, 4)))
    out_weight = normal_values(key_of[1], (SECTIONS, HD, N_MP, N_DP, DB), HD ** -0.5, 0.078125, ((0, 4), (1, 4), (3, 2)))
    residual = normal_values(key_of[2], (SECTIONS, TOK, D), 1.0, 6.0, ((0, 4), (2, 8)))
    layer_norm_gain = jnp.clip(1.0 + 0.15 * jax.random.normal(key_of[3], (SECTIONS, D), jnp.float32), 0.25, 1.75)
    layer_norm_bias = normal_values(key_of[4], (SECTIONS, D), 0.5, 3.0, ((0, 4), (1, 4)), jnp.float32)
    ln_cotangent = normal_values(key_of[5], (SECTIONS, TOK, D), 1.0, 6.0, ((0, 4), (1, 2), (2, 4)))
    return {"context": context, "out_weight": out_weight, "residual": residual, "layer_norm_gain": layer_norm_gain, "layer_norm_bias": layer_norm_bias, "ln_cotangent": ln_cotangent}


epsilon = 1e-05

def reference(context, out_weight, residual, layer_norm_gain, layer_norm_bias, ln_cotangent):
    weights = out_weight.reshape(SECTIONS, HD, D)

    def project(items):
        part_ctx, part_w, part_res = items
        summed = jnp.dot(part_ctx, part_w, preferred_element_type=jnp.float32)
        return (part_res.astype(jnp.float32) + summed).astype(jnp.bfloat16)
    section_out = lax.map(project, (context, weights, residual))
    arrived = jnp.roll(section_out, 1, axis=0).astype(jnp.float32)
    average = lax.optimization_barrier(jnp.mean(arrived, axis=-1, keepdims=True))
    centered_input = arrived - average
    variance = lax.optimization_barrier(jnp.mean(centered_input * centered_input, axis=-1, keepdims=True))
    inverse_deviation = lax.rsqrt(variance + epsilon)
    normalized_input = centered_input * inverse_deviation
    layer_norm_output = (normalized_input * layer_norm_gain[:, None, :] + layer_norm_bias[:, None, :]).astype(jnp.bfloat16)
    gain_scaled = ln_cotangent.astype(jnp.float32) * layer_norm_gain[:, None, :]
    input_mean = lax.optimization_barrier(jnp.mean(gain_scaled, axis=-1, keepdims=True))
    squared_mean = lax.optimization_barrier(jnp.mean(gain_scaled * normalized_input, axis=-1, keepdims=True))
    incoming_gradient = (inverse_deviation * (gain_scaled - input_mean - normalized_input * squared_mean)).astype(jnp.bfloat16)
    resid_grad = jnp.roll(incoming_gradient, -1, axis=0)
    return (layer_norm_output, resid_grad)
```

```python
import jax
import jax.numpy as jnp
from jax import lax
from jax.sharding import PartitionSpec as P


epsilon = 1e-05
CHUNKS = 4


def passed_along(x, axis, by):
    devices = lax.axis_size(axis)
    return lax.ppermute(x, axis, [(i, (i + by) % devices) for i in range(devices)])


def pick(x, index, axis=0):
    return lax.dynamic_index_in_dim(x, index, axis, keepdims=False)


def head_sum(part):
    n_mp = lax.axis_size("mp")
    me = lax.axis_index("mp")
    groups, core, group = n_mp // 2, me % 2, me // 2
    pairs = part.reshape(groups, 2, *part.shape[1:])
    away = pick(pairs, 1 - core, 1).astype(jnp.bfloat16)
    near = lax.ppermute(away, "mp", [(i, i ^ 1) for i in range(n_mp)])
    both = pick(pairs, core, 1) + near.astype(jnp.float32)
    total = pick(both, group)
    for k in range(1, groups):
        send = pick(both, (group + k) % groups).astype(jnp.bfloat16)
        got = lax.ppermute(
            send, "mp", [(i, ((i // 2 + k) % groups) * 2 + i % 2) for i in range(n_mp)]
        )
        total = total + got.astype(jnp.float32)
    return total


def relayout(values):
    n_dp, _, _ = values.shape
    if n_dp != 2:
        out = lax.all_to_all(values, "dp", split_axis=0, concat_axis=2, tiled=True)
        return out[0]
    me = lax.axis_index("dp")
    own = pick(values, me)
    got = lax.ppermute(pick(values, 1 - me), "dp", [(0, 1), (1, 0)])
    first = me == 0
    return jnp.concatenate([jnp.where(first, own, got), jnp.where(first, got, own)], axis=1)


def local(context, out_weight, residual, layer_norm_gain, layer_norm_bias, ln_cotangent):
    n_dp = lax.axis_size("dp")
    n_mp = lax.axis_size("mp")
    cotangent = passed_along(ln_cotangent[0], "section", -1)
    next_gain = passed_along(layer_norm_gain, "section", -1)
    weights = out_weight[0]
    weights = weights.reshape(weights.shape[0], weights.shape[1], weights.shape[3])
    tokens, heads = context.shape[1:]
    features = weights.shape[2]
    per = tokens // n_dp // CHUNKS
    local_ctx = context[0].reshape(n_dp, CHUNKS, per, heads)
    local_res = residual[0].reshape(n_dp, CHUNKS, per, features)

    blocks, arrived = [], []
    for c in range(CHUNKS):
        rows = local_ctx[:, c].reshape(n_dp * per, heads)
        part = jnp.einsum("th,hjr->jtr", rows, weights, preferred_element_type=jnp.float32)
        summed = head_sum(part)
        res = local_res[:, c].reshape(n_dp * per, features)
        section_out = (res.astype(jnp.float32) + summed).astype(jnp.bfloat16)
        block = relayout(section_out.reshape(n_dp, per, features))
        blocks.append(block)
        arrived.append(passed_along(block, "section", 1))

    width = float(n_mp * n_dp * features)
    sums = []
    for c in range(CHUNKS):
        x = blocks[c].astype(jnp.float32)
        g = cotangent[c * per:(c + 1) * per].astype(jnp.float32) * next_gain
        sums.append(
            jnp.stack([jnp.sum(x, -1), jnp.sum(x * x, -1), jnp.sum(g, -1), jnp.sum(g * x, -1)])
        )
    sums = lax.psum(jnp.concatenate(sums, axis=1), "mp")
    average = sums[0] / width
    variance = sums[1] / width - average * average
    inverse_deviation = lax.rsqrt(variance + epsilon)
    input_mean = sums[2] / width
    squared_mean = inverse_deviation * (sums[3] / width - average * input_mean)
    there = passed_along(jnp.stack([average, inverse_deviation]), "section", 1)

    grads, outs = [], []
    for c in range(CHUNKS):
        rows = slice(c * per, (c + 1) * per)
        x = blocks[c].astype(jnp.float32)
        g = cotangent[rows].astype(jnp.float32) * next_gain
        rstd = inverse_deviation[rows][:, None]
        xhat = (x - average[rows][:, None]) * rstd
        grads.append(
            (rstd * (g - input_mean[rows][:, None] - xhat * squared_mean[rows][:, None])).astype(
                jnp.bfloat16
            )
        )
        y = arrived[c].astype(jnp.float32)
        yhat = (y - there[0, rows][:, None]) * there[1, rows][:, None]
        outs.append((yhat * layer_norm_gain + layer_norm_bias).astype(jnp.bfloat16))
    return (jnp.concatenate(outs)[None], jnp.concatenate(grads)[None])


def solution(mesh):
    in_specs = (
        P("section", None, "mp"),
        P("section", "mp", None, "dp", None),
        P("section", None, ("mp", "dp")),
        P("section", "mp"),
        P("section", "mp"),
        P("section", "dp", "mp"),
    )
    out_specs = (P("section", "dp", "mp"), P("section", "dp", "mp"))
    return jax.shard_map(local, mesh=mesh, in_specs=in_specs, out_specs=out_specs, check_vma=False)
```
